256 devices in a mesh: gx: 8 (over z), gy: 4 (over x), gz: 8 (over y, core).
Axes of the slice: x: 4, y: 4, z: 8, core: 2. Of those that a mesh axis runs over, the one named last changes fastest.
Arguments:
- params: float32 [59, 524288], P(None, ('gx', 'gy', 'gz')), may hold values from -6 to 6
- gradients: float32 [59, 524288], P(None, ('gx', 'gy', 'gz')), may hold values from -80 to 80
- moment_one: float32 [59, 524288], P(None, ('gx', 'gy', 'gz')), may hold values from -4 to 4
- moment_two: float32 [59, 524288], P(None, ('gx', 'gy', 'gz')), may hold values from 0.01 to 1
- keep_mask: int32 [524288], P(('gx', 'gy', 'gz')), may hold values from 0 to 1, as said below
Outputs:
- new_params: float32 [59, 524288], P(None, ('gx', 'gy', 'gz'))
- new_moment_one: float32 [59, 524288], P(None, ('gx', 'gy', 'gz'))
- new_moment_two: float32 [59, 524288], P(None, ('gx', 'gy', 'gz'))
- grad_rms: float32 [], replicated
The draws below stay inside these ranges and needn't reach their ends.
Inputs may be any that keep to these rules, and one draw needn't show every extreme that they name: `keep_mask`: exactly 32 of the blocks of 128 aligned columns hold no 1; every other block holds at least one.
All inputs are finite; a program needn't handle non-finite values.
Results may differ from the reference program's by a relative error of at most 0.000067.
Values sent between devices are 32-bit elements; how exact they have to be, the bound alone decides.
No kernel may reach another device: no remote copies, remote signals or barrier semaphores. Data moves between devices by JAX's collectives and lax.ppermute only.
A program may use at most 64 MiB of HBM per device.

```python
import math
import jax
import jax.numpy as jnp
from jax import lax

FEATURES = 59
BLOCK = 128
STEP = 10
ROWS_DEV = 2048
ROWS = 524288
DROPS = 32


def draw_gradients(key, part):
    first_key, second_key = jax.random.split(jax.random.fold_in(key, 11), 2)
    position = jnp.arange(ROWS, dtype=jnp.float32) / ROWS
    rough = jnp.exp(jax.random.uniform(second_key, (ROWS,), jnp.float32, -0.7, 0.7))
    values = jax.random.truncated_normal(first_key, -4.0, 4.0, (FEATURES, ROWS), jnp.float32)
    scale = jnp.exp(jnp.log(3.0) * position) * rough
    return (values * scale[None, :]).astype(jnp.float32)


def draw_keep_mask(key, part):
    first_key, second_key, third_key, fourth_key, fifth_key = jax.random.split(jax.random.fold_in(key, 23), 5)
    total_blocks = ROWS // BLOCK
    blocks_dev = ROWS_DEV // BLOCK
    device_count = ROWS // ROWS_DEV
    ordering = jax.random.permutation(first_key, total_blocks).astype(jnp.int32)
    first_block = jax.random.randint(fourth_key, (), 0, blocks_dev).astype(jnp.int32)
    middle_block = (device_count // 2 * blocks_dev + jax.random.randint(fifth_key, (), 0, blocks_dev)).astype(jnp.int32)
    held = ordering[first_block]
    ordering = jnp.where(ordering == 0, held, ordering)
    ordering = ordering.at[first_block].set(0)
    held = ordering[middle_block]
    ordering = jnp.where(ordering == 1, held, ordering)
    ordering = ordering.at[middle_block].set(1)
    emptied = ordering < DROPS
    coins = jax.random.randint(second_key, (total_blocks, BLOCK), 0, 10) < 7
    chosen = jax.random.randint(third_key, (total_blocks, 1), 0, BLOCK)
    within = jnp.arange(BLOCK, dtype=jnp.int32)[None, :]
    survive = (coins | (within == chosen)) & jnp.logical_not(emptied)[:, None]
    return survive.astype(jnp.int32).reshape(ROWS)


def block_scale(stream_key, shape, cuts, low, top_value):
    def one(axis_at, blocks):
        heights = jax.random.uniform(jax.random.fold_in(jax.random.fold_in(stream_key, 6), axis_at), (blocks,), jnp.float32, low / len(cuts), top_value / len(cuts))
        return jnp.repeat(jnp.exp(heights), shape[axis_at] // blocks).reshape((-1,) + (1,) * (len(shape) - axis_at - 1))

    gain = one(*cuts[0])
    for cut in cuts[1:]:
        gain = gain * one(*cut)
    return gain


def scatter_about(rng, dims, scale, limit, shards=(), kind=jnp.bfloat16):
    values = jax.random.normal(rng, dims, jnp.float32) * scale
    if len(shards) > 0:
        values = block_scale(rng, dims, shards, -0.22, 0.18) * values
    return jnp.clip(values, min=-limit, max=limit).astype(kind)


def setup_inputs(seed: int = 0) -> dict:
    keys = jax.random.split(jax.random.key(seed), 6)
    return {
        "params": scatter_about(keys[0], (FEATURES, ROWS), 1.0, 6.0, ((1, 256),), jnp.float32),
        "gradients": draw_gradients(jax.random.fold_in(keys[5], 71), 0),
        "moment_one": scatter_about(keys[2], (FEATURES, ROWS), 0.3, 4.0, ((1, 256),), jnp.float32),
        "moment_two": jnp.clip(jnp.exp(math.log(1.0) - 4.6051702 * jax.random.uniform(keys[3], (FEATURES, ROWS), jnp.float32) ** block_scale(keys[3], (FEATURES, ROWS), ((1, 256),), -0.2, 0.2)), 0.01, 1.0),
        "keep_mask": draw_keep_mask(jax.random.fold_in(keys[5], 71), 0),
    }


beta_one = 0.9
beta_two = 0.999
learn_rate = 0.05
adam_eps = 1e-08
clip_rms = 1.0

def adam_update(params, gradients, moment_one, moment_two, clip_factor):
    clipped = clip_factor * gradients
    first = beta_one * moment_one + (1.0 - beta_one) * clipped
    second = beta_two * moment_two + (1.0 - beta_two) * clipped * clipped
    correct_one = 1.0 - beta_one ** STEP
    correct_two = 1.0 - beta_two ** STEP
    updated = params - learn_rate * (first / correct_one) / (jnp.sqrt(second / correct_two) + adam_eps)
    return (updated, first, second)

def reference(params, gradients, moment_one, moment_two, keep_mask):
    square_total = jnp.sum(gradients * gradients)
    grad_rms = jnp.sqrt(square_total / (FEATURES * ROWS))
    clip_factor = jnp.minimum(1.0, clip_rms / (grad_rms + 1e-06))
    updated, first, second = adam_update(params, gradients, moment_one, moment_two, clip_factor)
    stacked = jnp.stack([updated, first, second])
    stacked = jnp.where(keep_mask[None, None, :] > 0, stacked, 0.0)
    total_blocks = ROWS // BLOCK
    counts = lax.optimization_barrier(jnp.sum(keep_mask.reshape(total_blocks, BLOCK), axis=1))
    block_alive = (counts > 0).astype(jnp.int32)
    block_rank = (jnp.cumsum(block_alive) - block_alive).astype(jnp.int32)
    target_block = jnp.where(block_alive > 0, block_rank, total_blocks).astype(jnp.int32)
    blocked = stacked.reshape(3, FEATURES, total_blocks, BLOCK)
    result = jnp.zeros_like(blocked).at[:, :, target_block].set(blocked, mode='drop')
    result = result.reshape(3, FEATURES, ROWS)
    return (result[0], result[1], result[2], grad_rms)
```

```python
import functools

import jax
import jax.numpy as jnp
from jax import lax
from jax.experimental import pallas as pl
from jax.experimental.pallas import tpu as pltpu
from jax.sharding import Mesh
from jax.sharding import PartitionSpec as P

FEATURES = 59
BLOCK = 128
STEP = 10
AXES = ("gx", "gy", "gz_0", "gz_1")

beta_one = 0.9
beta_two = 0.999
learn_rate = 0.05
adam_eps = 1e-08
clip_rms = 1.0
correct_one = 1.0 - beta_one**STEP
correct_two = 1.0 - beta_two**STEP


def from_next_chip(x):
    size = lax.axis_size(AXES)
    return lax.ppermute(x, AXES, [(i, i - 2) for i in range(2, size)])


def swap_cores(x):
    return lax.ppermute(x, "gz_1", [(0, 1), (1, 0)])


def sent_to_all(x, axes):
    size = lax.axis_size(axes)
    return lax.all_to_all(jnp.broadcast_to(x[None], (size, *x.shape)), axes, 0, 0, tiled=True)


def final_kernel(index, valid, po, ps, pr, vo, vs, vr, mo, ms, mr, p_out, m_out, v_out):
    for slot in range(p_out.shape[1] // BLOCK):
        place = index[slot]
        part = place // 16
        lanes = pl.ds(pl.multiple_of((place % 16) * BLOCK, BLOCK), BLOCK)
        here = pl.ds(slot * BLOCK, BLOCK)

        def pick(own, swapped, received):
            later = jnp.where(part == 1, swapped[:, lanes], received[:, lanes])
            return jnp.where(valid[slot] > 0, jnp.where(part == 0, own[:, lanes], later), 0.0)

        first = pick(mo, ms, mr)
        second = pick(vo, vs, vr)
        m_out[:, here] = first
        v_out[:, here] = second
        p_out[:, here] = pick(po, ps, pr) - learn_rate * (first / correct_one) / (
            jnp.sqrt(second / correct_two) + adam_eps
        )


def shards(params, gradients, moment_one, moment_two, keep_mask):
    rows = params.shape[1]
    blocks = rows // BLOCK
    devices = lax.axis_size(AXES)
    core = lax.axis_index("gz_1")
    kept = keep_mask[None, :] > 0

    alive = (jnp.max(keep_mask.reshape(blocks, BLOCK), axis=1) > 0).astype(jnp.int32)
    pair = jnp.stack([jnp.sum(gradients * gradients), jnp.sum(alive).astype(jnp.float32)])
    near = ("gz_0", "gz_1")
    far = ("gx", "gy")
    near_pairs = sent_to_all(pair, near)
    near_lower = jnp.arange(8) < lax.axis_index(near)
    far_pairs = sent_to_all(jnp.sum(near_pairs, axis=0), far)
    far_lower = jnp.arange(32) < lax.axis_index(far)
    lower = jnp.sum(jnp.where(near_lower, near_pairs[:, 1], 0.0)) + jnp.sum(
        jnp.where(far_lower, far_pairs[:, 1], 0.0)
    )
    offset = lower.astype(jnp.int32)
    grad_rms = jnp.sqrt(jnp.sum(far_pairs[:, 0]) / (FEATURES * rows * devices))
    clip_factor = jnp.minimum(1.0, clip_rms / (grad_rms + 1e-06))

    def window(own):
        received = from_next_chip(own)
        swapped = swap_cores(jnp.where(core == 0, received, own))
        return own, swapped, received

    p_window = window(jnp.where(kept, params, 0.0))
    clipped = clip_factor * gradients
    first = jnp.where(kept, beta_one * moment_one + (1.0 - beta_one) * clipped, 0.0)
    second = jnp.where(
        kept, beta_two * moment_two + (1.0 - beta_two) * clipped * clipped, 0.0
    )
    v_window = window(second)
    m_window = window(first)

    def alive_in(x):
        return (jnp.max(x[0].reshape(blocks, BLOCK), axis=1) > 0).astype(jnp.int32)

    flags = jnp.concatenate([alive, alive_in(v_window[1]), alive_in(v_window[2])])
    place = jnp.arange(3 * blocks)
    rank = jnp.sum(jnp.where(place[:, None] < place[None, :], flags[:, None], 0), axis=0)
    wanted = lax.axis_index(AXES) * blocks - offset + jnp.arange(blocks)
    match = (rank[None, :] == wanted[:, None]) & (flags[None, :] > 0)
    index = jnp.sum(jnp.where(match, place[None, :], 0), axis=1)
    valid = jnp.sum(match.astype(jnp.int32), axis=1)

    smem = pl.BlockSpec(memory_space=pltpu.SMEM)
    vmem = pl.BlockSpec(memory_space=pltpu.VMEM)
    out = jax.ShapeDtypeStruct(params.shape, jnp.float32)
    p1, m1, v1 = pl.pallas_call(
        final_kernel,
        out_shape=(out, out, out),
        in_specs=[smem, smem] + [vmem] * 9,
        out_specs=(vmem, vmem, vmem),
        name="compact",
    )(index, valid, *p_window, *v_window, *m_window)
    return p1, m1, v1, grad_rms


def solution(mesh):
    split = Mesh(
        mesh.devices.reshape(mesh.shape["gx"], mesh.shape["gy"], 4, 2), AXES
    )
    spec = P(None, AXES)
    return jax.shard_map(
        shards,
        mesh=split,
        in_specs=(spec, spec, spec, spec, P(AXES)),
        out_specs=(spec, spec, spec, P()),
        check_vma=False,
    )
```

```python
import jax
import jax.numpy as jnp
from jax import lax
from jax.experimental import pallas as pl
from jax.experimental.pallas import tpu as pltpu
from jax.sharding import Mesh
from jax.sharding import PartitionSpec as P


FEATURES = 59
BLOCK = 128
BLOCKS = 16
STEP = 10
DEVICES = 256
AXES = ("gx", "gy", "gz_0", "gz_1")
NEAR = ("gz_0", "gz_1")
FAR = ("gx", "gy")
CHUNKS = ((0, 24), (24, 24), (48, 11))

beta_one = 0.9
beta_two = 0.999
learn_rate = 0.05
adam_eps = 1e-08
clip_rms = 1.0
correct_one = 1.0 - beta_one**STEP
correct_two = 1.0 - beta_two**STEP

ANY = pl.BlockSpec(memory_space=pl.ANY)
SMEM = pl.BlockSpec(memory_space=pltpu.SMEM)
VMEM = pl.BlockSpec(memory_space=pltpu.VMEM)


def pack_kernel(p_ref, g_ref, m_ref, v_ref, mask_ref, pair_ref, *chunks):
    grads = g_ref[...]
    square = jnp.sum(grads * grads)
    alive = (jnp.max(mask_ref[...], axis=1, keepdims=True) > 0).astype(jnp.float32)
    lane = lax.broadcasted_iota(jnp.int32, (BLOCKS, BLOCK), 1)
    block = lax.broadcasted_iota(jnp.int32, (BLOCKS, BLOCK), 0)
    chosen = (lane == block + 2) | (lane == 1)
    row = jnp.sum(jnp.where(chosen, alive, 0.0), axis=0, keepdims=True)
    first_lane = lax.broadcasted_iota(jnp.int32, (1, BLOCK), 1)
    row = jnp.where(first_lane == 0, square, row)
    pair_ref[...] = jnp.broadcast_to(row[None], pair_ref.shape)
    for (start, count), out in zip(CHUNKS, chunks):
        rows = slice(start, start + count)
        out[0:count, :] = p_ref[rows, :]
        out[count : 2 * count, :] = g_ref[rows, :]
        out[2 * count : 3 * count, :] = m_ref[rows, :]
    for b in range(BLOCKS):
        here = slice(b * BLOCK, (b + 1) * BLOCK)
        kept = mask_ref[b : b + 1, :] > 0
        for (start, count), out in zip(CHUNKS, chunks):
            value = v_ref[start : start + count, here]
            out[3 * count : 4 * count, here] = jnp.where(kept, value, 0.0)


def line_kernel(near_ref, far_ref):
    near = near_ref[:, 0, :]
    lane = lax.broadcasted_iota(jnp.int32, (1, BLOCK), 1)
    total = jnp.sum(near, axis=0, keepdims=True)
    second = pltpu.roll(near[1:2], BLOCKS, 1)
    row = jnp.where(lane < 2 + BLOCKS, near[0:1], second)
    row = jnp.where(lane < 2, total, jnp.where(lane < 2 + 2 * BLOCKS, row, 0.0))
    far_ref[...] = jnp.broadcast_to(row[None], far_ref.shape)


def table_kernel(near_ref, far_ref, place_ref, scale_ref):
    y_core = lax.axis_index("gz_0") * 2 + lax.axis_index("gz_1")
    line = lax.axis_index("gx") * 4 + lax.axis_index("gy")
    near = near_ref[:, 0, :]
    far = far_ref[:, 0, :]
    near_row = lax.broadcasted_iota(jnp.int32, near.shape, 0)
    far_row = lax.broadcasted_iota(jnp.int32, far.shape, 0)
    lane = lax.broadcasted_iota(jnp.int32, (1, BLOCK), 1)

    lower = jnp.sum(jnp.where(near_row < y_core, near, 0.0), axis=0, keepdims=True)
    lower += jnp.sum(jnp.where(far_row < line, far, 0.0), axis=0, keepdims=True)
    lower = jnp.sum(jnp.where(lane == 1, lower, 0.0), axis=1, keepdims=True)
    total = jnp.sum(far, axis=0, keepdims=True)
    total = jnp.sum(jnp.where(lane == 0, total, 0.0), axis=1, keepdims=True)
    rms = jnp.sqrt(total / (FEATURES * BLOCKS * BLOCK * DEVICES))
    clip = jnp.minimum(1.0, clip_rms / (rms + 1e-06))
    scale_ref[...] = jnp.where(lane == 0, clip, rms)

    def near_flags(device):
        return jnp.sum(jnp.where(near_row == device, near, 0.0), axis=0, keepdims=True)

    after = jnp.sum(jnp.where(far_row == line + 1, far, 0.0), axis=0, keepdims=True)
    later = pltpu.roll(after, BLOCK - BLOCKS, 1)
    own = near_flags(y_core)
    middle = jnp.where(y_core < 7, near_flags(y_core + 1), after)
    last = jnp.where(y_core < 6, near_flags(y_core + 2), jnp.where(y_core == 6, after, later))
    flags = jnp.where(
        lane < BLOCKS,
        pltpu.roll(own, BLOCK - 2, 1),
        jnp.where(
            lane < 2 * BLOCKS, pltpu.roll(middle, BLOCKS - 2, 1), pltpu.roll(last, 2 * BLOCKS - 2, 1)
        ),
    )
    window = (3 * BLOCKS, BLOCK)
    flags = jnp.broadcast_to(flags, window)
    row = lax.broadcasted_iota(jnp.int32, window, 0)
    column = lax.broadcasted_iota(jnp.int32, window, 1)
    rank = jnp.sum(jnp.where(column < row, flags, 0.0), axis=1, keepdims=True)
    alive = jnp.sum(jnp.where(column == row, flags, 0.0), axis=1, keepdims=True)
    device = line * 8 + y_core
    wanted = (device * BLOCKS).astype(jnp.float32) - lower + column.astype(jnp.float32)
    match = (rank == wanted) & (alive > 0.0)
    place = jnp.sum(jnp.where(match, row + 1, 0), axis=0, keepdims=True)
    place_ref[...] = place


def update_kernel(start, count, place, scale, own, below, above, received, *refs):
    p_all, m_all, v_all, block, p_rows, m_rows, v_rows, sems, out_sems = refs[-9:]
    core = lax.axis_index("gz_1")

    def landing(slot):
        return block.at[:, pl.ds(slot * BLOCK, BLOCK)]

    for slot in range(BLOCKS):
        at = jnp.maximum(place[0, slot] - 1, 0)
        part = at // BLOCKS
        lanes = pl.ds(pl.multiple_of((at % BLOCKS) * BLOCK, BLOCK), BLOCK)
        cases = (
            (part == 0, own),
            ((part == 1) & (core == 0), below),
            ((part == 1) & (core == 1), above),
            (part == 2, received),
        )
        for condition, ref in cases:

            @pl.when(condition)
            def _(ref=ref, lanes=lanes, slot=slot):
                pltpu.make_async_copy(ref.at[:, lanes], landing(slot), sems.at[slot]).start()

    factor = scale[0, 0]
    for slot in range(BLOCKS):
        here = pl.ds(slot * BLOCK, BLOCK)
        pltpu.make_async_copy(own.at[:, pl.ds(0, BLOCK)], landing(slot), sems.at[slot]).wait()
        second = block[3 * count : 4 * count, here]
        kept = (second > 0.0) & (place[0, slot] > 0)
        clipped = factor * block[count : 2 * count, here]
        first = beta_one * block[2 * count : 3 * count, here] + (1.0 - beta_one) * clipped
        second = beta_two * second + (1.0 - beta_two) * clipped * clipped
        updated = block[0:count, here] - learn_rate * (first / correct_one) / (
            jnp.sqrt(second / correct_two) + adam_eps
        )
        p_rows[:, here] = jnp.where(kept, updated, 0.0)
        m_rows[:, here] = jnp.where(kept, first, 0.0)
        v_rows[:, here] = jnp.where(kept, second, 0.0)
    rows = pl.ds(start, count)
    copies = [
        pltpu.make_async_copy(rows_ref, whole.at[rows, :], out_sems.at[i])
        for i, (rows_ref, whole) in enumerate(((p_rows, p_all), (m_rows, m_all), (v_rows, v_all)))
    ]
    for copy in copies:
        copy.start()
    for copy in copies:
        copy.wait()


def update_rows(start, count, place, scale, parts, outs, out_type):
    operands = (place, scale, *parts, *outs)
    return pl.pallas_call(
        lambda *refs: update_kernel(start, count, *refs),
        out_shape=(out_type,) * 3,
        in_specs=[SMEM, SMEM] + [ANY] * (len(operands) - 2),
        out_specs=(ANY,) * 3,
        input_output_aliases={6 + i: i for i in range(len(outs))},
        scratch_shapes=[
            pltpu.VMEM((4 * count, BLOCKS * BLOCK), jnp.float32),
            *[pltpu.VMEM((count, BLOCKS * BLOCK), jnp.float32)] * 3,
            pltpu.SemaphoreType.DMA((BLOCKS,)),
            pltpu.SemaphoreType.DMA((3,)),
        ],
        cost_estimate=pl.CostEstimate(flops=10000000, bytes_accessed=2000000, transcendentals=0),
        name="update",
    )(*operands)


def shards(params, gradients, moment_one, moment_two, keep_mask):
    row_count = params.shape[1]
    f32 = jnp.float32
    pairs, *own = pl.pallas_call(
        pack_kernel,
        out_shape=(
            jax.ShapeDtypeStruct((8, 1, BLOCK), f32),
            *[jax.ShapeDtypeStruct((4 * count, row_count), f32) for _, count in CHUNKS],
        ),
        in_specs=[VMEM] * 5,
        out_specs=(VMEM,) * (1 + len(CHUNKS)),
        name="pack",
    )(params, gradients, moment_one, moment_two, keep_mask.reshape(BLOCKS, BLOCK))

    near = lax.all_to_all(pairs, NEAR, 0, 0, tiled=True)
    lines = pl.pallas_call(
        line_kernel,
        out_shape=jax.ShapeDtypeStruct((32, 1, BLOCK), f32),
        name="line",
    )(near)
    far = lax.all_to_all(lines, FAR, 0, 0, tiled=True)
    place, scale = pl.pallas_call(
        table_kernel,
        out_shape=(
            jax.ShapeDtypeStruct((1, BLOCK), jnp.int32),
            jax.ShapeDtypeStruct((1, BLOCK), f32),
        ),
        name="table",
    )(near, far)

    out_type = jax.ShapeDtypeStruct(params.shape, f32)
    outs = ()
    for i, (start, count) in enumerate(CHUNKS):
        received = lax.ppermute(own[i], AXES, [(d, d - 2) for d in range(2, DEVICES)])
        below = lax.ppermute(own[i], "gz_1", [(1, 0)])
        above = lax.ppermute(received, "gz_1", [(0, 1)])
        parts = (own[i], below, above, received)
        outs = update_rows(start, count, place, scale, parts, outs, out_type)
    return (*outs, scale[0, 1])


def solution(mesh):
    split = Mesh(mesh.devices.reshape(mesh.shape["gx"], mesh.shape["gy"], 4, 2), AXES)
    spec = P(None, AXES)

    return jax.shard_map(
        shards,
        mesh=split,
        in_specs=(spec, spec, spec, spec, P(AXES)),
        out_specs=(spec, spec, spec, P()),
        check_vma=False,
    )
```

```python
import jax
import jax.numpy as jnp
from jax import lax
from jax.experimental import pallas as pl
from jax.experimental.pallas import tpu as pltpu
from jax.sharding import Mesh
from jax.sharding import PartitionSpec as P


FEATURES = 59
BLOCK = 128
BLOCKS = 16
STEP = 10
DEVICES = 256
AXES = ("gx", "gy", "gz_0", "gz_1")
NEAR = ("gz_0", "gz_1")
FAR = ("gx", "gy")
CHUNKS = ((24, 35), (0, 24))

beta_one = 0.9
beta_two = 0.999
learn_rate = 0.05
adam_eps = 1e-08
clip_rms = 1.0
correct_one = 1.0 - beta_one**STEP
correct_two = 1.0 - beta_two**STEP

ANY = pl.BlockSpec(memory_space=pl.ANY)
SMEM = pl.BlockSpec(memory_space=pltpu.SMEM)
VMEM = pl.BlockSpec(memory_space=pltpu.VMEM)


def pack_kernel(g_ref, m_ref, v_ref, mask_ref, pair_ref, *chunks):
    grads = g_ref[...]
    square = jnp.sum(grads * grads)
    alive = (jnp.max(mask_ref[...], axis=1, keepdims=True) > 0).astype(jnp.float32)
    lane = lax.broadcasted_iota(jnp.int32, (BLOCKS, BLOCK), 1)
    block = lax.broadcasted_iota(jnp.int32, (BLOCKS, BLOCK), 0)
    chosen = (lane == block + 2) | (lane == 1)
    row = jnp.sum(jnp.where(chosen, alive, 0.0), axis=0, keepdims=True)
    first_lane = lax.broadcasted_iota(jnp.int32, (1, BLOCK), 1)
    row = jnp.where(first_lane == 0, square, row)
    pair_ref[...] = jnp.broadcast_to(row[None], pair_ref.shape)
    for (start, count), out in zip(CHUNKS, chunks):
        rows = slice(start, start + count)
        out[0:count, :] = g_ref[rows, :]
        out[count : 2 * count, :] = m_ref[rows, :]
    for b in range(BLOCKS):
        here = slice(b * BLOCK, (b + 1) * BLOCK)
        kept = mask_ref[b : b + 1, :] > 0
        for (start, count), out in zip(CHUNKS, chunks):
            value = v_ref[start : start + count, here]
            out[2 * count : 3 * count, here] = jnp.where(kept, value, 0.0)


def line_kernel(near_ref, far_ref):
    near = near_ref[:, 0, :]
    lane = lax.broadcasted_iota(jnp.int32, (1, BLOCK), 1)
    total = jnp.sum(near, axis=0, keepdims=True)
    second = pltpu.roll(near[1:2], BLOCKS, 1)
    row = jnp.where(lane < 2 + BLOCKS, near[0:1], second)
    row = jnp.where(lane < 2, total, jnp.where(lane < 2 + 2 * BLOCKS, row, 0.0))
    far_ref[...] = jnp.broadcast_to(row[None], far_ref.shape)


def table_kernel(near_ref, far_ref, place_ref, clip_ref, rms_ref):
    y_core = lax.axis_index("gz_0") * 2 + lax.axis_index("gz_1")
    line = lax.axis_index("gx") * 4 + lax.axis_index("gy")
    near = near_ref[:, 0, :]
    far = far_ref[:, 0, :]
    near_row = lax.broadcasted_iota(jnp.int32, near.shape, 0)
    far_row = lax.broadcasted_iota(jnp.int32, far.shape, 0)
    lane = lax.broadcasted_iota(jnp.int32, (1, BLOCK), 1)

    lower = jnp.sum(jnp.where(near_row < y_core, near, 0.0), axis=0, keepdims=True)
    lower += jnp.sum(jnp.where(far_row < line, far, 0.0), axis=0, keepdims=True)
    lower = jnp.sum(jnp.where(lane == 1, lower, 0.0), axis=1, keepdims=True)
    total = jnp.sum(far, axis=0, keepdims=True)
    total = jnp.sum(jnp.where(lane == 0, total, 0.0), axis=1, keepdims=True)
    rms = jnp.sqrt(total / (FEATURES * BLOCKS * BLOCK * DEVICES))
    clip = jnp.minimum(1.0, clip_rms / (rms + 1e-06))
    clip_ref[...] = jnp.broadcast_to(clip, clip_ref.shape)
    rms_ref[...] = rms

    def near_flags(device):
        return jnp.sum(jnp.where(near_row == device, near, 0.0), axis=0, keepdims=True)

    after = jnp.sum(jnp.where(far_row == line + 1, far, 0.0), axis=0, keepdims=True)
    later = pltpu.roll(after, BLOCK - BLOCKS, 1)
    own = near_flags(y_core)
    middle = jnp.where(y_core < 7, near_flags(y_core + 1), after)
    last = jnp.where(y_core < 6, near_flags(y_core + 2), jnp.where(y_core == 6, after, later))
    flags = jnp.where(
        lane < BLOCKS,
        pltpu.roll(own, BLOCK - 2, 1),
        jnp.where(
            lane < 2 * BLOCKS, pltpu.roll(middle, BLOCKS - 2, 1), pltpu.roll(last, 2 * BLOCKS - 2, 1)
        ),
    )
    window = (3 * BLOCKS, BLOCK)
    flags = jnp.broadcast_to(flags, window)
    row = lax.broadcasted_iota(jnp.int32, window, 0)
    column = lax.broadcasted_iota(jnp.int32, window, 1)
    rank = jnp.sum(jnp.where(column < row, flags, 0.0), axis=1, keepdims=True)
    alive = jnp.sum(jnp.where(column == row, flags, 0.0), axis=1, keepdims=True)
    device = line * 8 + y_core
    wanted = (device * BLOCKS).astype(jnp.float32) - lower + column.astype(jnp.float32)
    match = (rank == wanted) & (alive > 0.0)
    place = jnp.sum(jnp.where(match, row + 1, 0), axis=0, keepdims=True)
    place_ref[...] = place


def update_kernel(start, count, place, clip, *refs):
    p_parts, parts = refs[0:4], refs[4:8]
    p_all, m_all, v_all, p_block, block, p_rows, m_rows, v_rows, sems, out_sems = refs[-10:]
    core = lax.axis_index("gz_1")
    rows = pl.ds(start, count)

    def copies(p_ref, ref, lanes, slot):
        here = pl.ds(slot * BLOCK, BLOCK)
        return (
            pltpu.make_async_copy(ref.at[:, lanes], block.at[:, here], sems.at[0, slot]),
            pltpu.make_async_copy(p_ref.at[rows, lanes], p_block.at[:, here], sems.at[1, slot]),
        )

    for slot in range(BLOCKS):
        at = jnp.maximum(place[0, slot] - 1, 0)
        part = at // BLOCKS
        lanes = pl.ds(pl.multiple_of((at % BLOCKS) * BLOCK, BLOCK), BLOCK)
        cases = (part == 0, (part == 1) & (core == 0), (part == 1) & (core == 1), part == 2)
        for condition, p_ref, ref in zip(cases, p_parts, parts):

            @pl.when(condition)
            def _(p_ref=p_ref, ref=ref, lanes=lanes, slot=slot):
                for copy in copies(p_ref, ref, lanes, slot):
                    copy.start()

    factor = clip[0, 0]
    for slot in range(BLOCKS):
        here = pl.ds(slot * BLOCK, BLOCK)
        for copy in copies(p_parts[0], parts[0], pl.ds(0, BLOCK), slot):
            copy.wait()
        second = block[2 * count : 3 * count, here]
        kept = (second > 0.0) & (place[0, slot] > 0)
        clipped = factor * block[0:count, here]
        first = beta_one * block[count : 2 * count, here] + (1.0 - beta_one) * clipped
        second = beta_two * second + (1.0 - beta_two) * clipped * clipped
        updated = p_block[:, here] - learn_rate * (first / correct_one) / (
            jnp.sqrt(second / correct_two) + adam_eps
        )
        p_rows[:, here] = jnp.where(kept, updated, 0.0)
        m_rows[:, here] = jnp.where(kept, first, 0.0)
        v_rows[:, here] = jnp.where(kept, second, 0.0)
    done = [
        pltpu.make_async_copy(rows_ref, whole.at[rows, :], out_sems.at[i])
        for i, (rows_ref, whole) in enumerate(((p_rows, p_all), (m_rows, m_all), (v_rows, v_all)))
    ]
    for copy in done:
        copy.start()
    for copy in done:
        copy.wait()


def update_rows(start, count, place, clip, p_parts, parts, outs, out_type):
    operands = (place, clip, *p_parts, *parts, *outs)
    width = BLOCKS * BLOCK
    return pl.pallas_call(
        lambda *refs: update_kernel(start, count, *refs),
        out_shape=(out_type,) * 3,
        in_specs=[SMEM, SMEM] + [ANY] * (len(operands) - 2),
        out_specs=(ANY,) * 3,
        input_output_aliases={10 + i: i for i in range(len(outs))},
        scratch_shapes=[
            pltpu.VMEM((count, width), jnp.float32),
            pltpu.VMEM((3 * count, width), jnp.float32),
            *[pltpu.VMEM((count, width), jnp.float32)] * 3,
            pltpu.SemaphoreType.DMA((2, BLOCKS)),
            pltpu.SemaphoreType.DMA((3,)),
        ],
        compiler_params=pltpu.CompilerParams(vmem_limit_bytes=8 * 1024 * 1024),
        cost_estimate=pl.CostEstimate(flops=10000000, bytes_accessed=2000000, transcendentals=0),
        name="update",
    )(*operands)


def shards(params, gradients, moment_one, moment_two, keep_mask):
    row_count = params.shape[1]
    f32 = jnp.float32
    small = pltpu.CompilerParams(vmem_limit_bytes=1024 * 1024)

    def moved(x):
        received = lax.ppermute(x, AXES, [(d, d - 2) for d in range(2, DEVICES)])
        below = lax.ppermute(x, "gz_1", [(1, 0)])
        above = lax.ppermute(received, "gz_1", [(0, 1)])
        return x, below, above, received

    pairs, *own = pl.pallas_call(
        pack_kernel,
        out_shape=(
            jax.ShapeDtypeStruct((8, 1, BLOCK), f32),
            *[jax.ShapeDtypeStruct((3 * count, row_count), f32) for _, count in CHUNKS],
        ),
        in_specs=[VMEM] * 4,
        out_specs=(VMEM,) * (1 + len(CHUNKS)),
        name="pack",
    )(gradients, moment_one, moment_two, keep_mask.reshape(BLOCKS, BLOCK))

    near = lax.all_to_all(pairs, NEAR, 0, 0, tiled=True)
    lines = pl.pallas_call(
        line_kernel,
        out_shape=jax.ShapeDtypeStruct((32, 1, BLOCK), f32),
        compiler_params=small,
        name="line",
    )(near)
    far = lax.all_to_all(lines, FAR, 0, 0, tiled=True)
    place, clip, rms = pl.pallas_call(
        table_kernel,
        out_shape=(
            jax.ShapeDtypeStruct((1, BLOCK), jnp.int32),
            jax.ShapeDtypeStruct((1, BLOCK), f32),
            jax.ShapeDtypeStruct((1, 1), f32),
        ),
        compiler_params=small,
        name="table",
    )(near, far)

    out_type = jax.ShapeDtypeStruct(params.shape, f32)
    p_parts = moved(params)
    outs = ()
    for i, (start, count) in enumerate(CHUNKS):
        parts = moved(own[i])
        outs = update_rows(start, count, place, clip, p_parts, parts, outs, out_type)
    return (*outs, rms.reshape(()))


def solution(mesh):
    split = Mesh(mesh.devices.reshape(mesh.shape["gx"], mesh.shape["gy"], 4, 2), AXES)
    spec = P(None, AXES)

    return jax.shard_map(
        shards,
        mesh=split,
        in_specs=(spec, spec, spec, spec, P(AXES)),
        out_specs=(spec, spec, spec, P()),
        check_vma=False,
    )
```

```python
import jax
import jax.numpy as jnp
from jax import lax
from jax.experimental import pallas as pl
from jax.experimental.pallas import tpu as pltpu
from jax.sharding import Mesh
from jax.sharding import PartitionSpec as P


FEATURES = 59
BLOCK = 128
BLOCKS = 16
STEP = 10
DEVICES = 256
AXES = ("gx", "gy", "gz_0", "gz_1")
NEAR = ("gz_0", "gz_1")
FAR = ("gx", "gy")
CHUNKS = ((32, 27), (0, 32))
LAST = "1"

beta_one = 0.9
beta_two = 0.999
learn_rate = 0.05
adam_eps = 1e-08
clip_rms = 1.0
correct_one = 1.0 - beta_one**STEP
correct_two = 1.0 - beta_two**STEP

ANY = pl.BlockSpec(memory_space=pl.ANY)
SMEM = pl.BlockSpec(memory_space=pltpu.SMEM)
VMEM = pl.BlockSpec(memory_space=pltpu.VMEM)


def pack_kernel(g_ref, m_ref, v_ref, mask_ref, pair_ref, *chunks):
    grads = g_ref[...]
    square = jnp.sum(grads * grads)
    alive = (jnp.max(mask_ref[...], axis=1, keepdims=True) > 0).astype(jnp.float32)
    lane = lax.broadcasted_iota(jnp.int32, (BLOCKS, BLOCK), 1)
    block = lax.broadcasted_iota(jnp.int32, (BLOCKS, BLOCK), 0)
    chosen = (lane == block + 2) | (lane == 1)
    row = jnp.sum(jnp.where(chosen, alive, 0.0), axis=0, keepdims=True)
    first_lane = lax.broadcasted_iota(jnp.int32, (1, BLOCK), 1)
    row = jnp.where(first_lane == 0, square, row)
    pair_ref[...] = jnp.broadcast_to(row[None], pair_ref.shape)
    for (start, count), out in zip(CHUNKS, chunks):
        rows = slice(start, start + count)
        out[0:count, :] = g_ref[rows, :]
        out[count : 2 * count, :] = m_ref[rows, :]
    for b in range(BLOCKS):
        here = slice(b * BLOCK, (b + 1) * BLOCK)
        kept = mask_ref[b : b + 1, :] > 0
        for (start, count), out in zip(CHUNKS, chunks):
            value = v_ref[start : start + count, here]
            out[2 * count : 3 * count, here] = jnp.where(kept, value, 0.0)


def line_kernel(near_ref, far_ref):
    near = near_ref[:, 0, :]
    lane = lax.broadcasted_iota(jnp.int32, (1, BLOCK), 1)
    total = jnp.sum(near, axis=0, keepdims=True)
    second = pltpu.roll(near[1:2], BLOCKS, 1)
    row = jnp.where(lane < 2 + BLOCKS, near[0:1], second)
    row = jnp.where(lane < 2, total, jnp.where(lane < 2 + 2 * BLOCKS, row, 0.0))
    far_ref[...] = jnp.broadcast_to(row[None], far_ref.shape)


def table_kernel(near_ref, far_ref, place_ref, clip_ref, rms_ref):
    y_core = lax.axis_index("gz_0") * 2 + lax.axis_index("gz_1")
    line = lax.axis_index("gx") * 4 + lax.axis_index("gy")
    near = near_ref[:, 0, :]
    far = far_ref[:, 0, :]
    near_row = lax.broadcasted_iota(jnp.int32, near.shape, 0)
    far_row = lax.broadcasted_iota(jnp.int32, far.shape, 0)
    lane = lax.broadcasted_iota(jnp.int32, (1, BLOCK), 1)

    lower = jnp.sum(jnp.where(near_row < y_core, near, 0.0), axis=0, keepdims=True)
    lower += jnp.sum(jnp.where(far_row < line, far, 0.0), axis=0, keepdims=True)
    lower = jnp.sum(jnp.where(lane == 1, lower, 0.0), axis=1, keepdims=True)
    total = jnp.sum(far, axis=0, keepdims=True)
    total = jnp.sum(jnp.where(lane == 0, total, 0.0), axis=1, keepdims=True)
    rms = jnp.sqrt(total / (FEATURES * BLOCKS * BLOCK * DEVICES))
    clip = jnp.minimum(1.0, clip_rms / (rms + 1e-06))
    clip_ref[...] = jnp.broadcast_to(clip, clip_ref.shape)
    rms_ref[...] = rms

    def near_flags(device):
        return jnp.sum(jnp.where(near_row == device, near, 0.0), axis=0, keepdims=True)

    after = jnp.sum(jnp.where(far_row == line + 1, far, 0.0), axis=0, keepdims=True)
    later = pltpu.roll(after, BLOCK - BLOCKS, 1)
    own = near_flags(y_core)
    middle = jnp.where(y_core < 7, near_flags(y_core + 1), after)
    last = jnp.where(y_core < 6, near_flags(y_core + 2), jnp.where(y_core == 6, after, later))
    flags = jnp.where(
        lane < BLOCKS,
        pltpu.roll(own, BLOCK - 2, 1),
        jnp.where(
            lane < 2 * BLOCKS, pltpu.roll(middle, BLOCKS - 2, 1), pltpu.roll(last, 2 * BLOCKS - 2, 1)
        ),
    )
    window = (3 * BLOCKS, BLOCK)
    flags = jnp.broadcast_to(flags, window)
    row = lax.broadcasted_iota(jnp.int32, window, 0)
    column = lax.broadcasted_iota(jnp.int32, window, 1)
    rank = jnp.sum(jnp.where(column < row, flags, 0.0), axis=1, keepdims=True)
    alive = jnp.sum(jnp.where(column == row, flags, 0.0), axis=1, keepdims=True)
    device = line * 8 + y_core
    wanted = (device * BLOCKS).astype(jnp.float32) - lower + column.astype(jnp.float32)
    match = (rank == wanted) & (alive > 0.0)
    place = jnp.sum(jnp.where(match, row + 1, 0), axis=0, keepdims=True)
    place_ref[...] = place


def update_kernel(start, count, place, clip, *refs):
    p_parts, parts = refs[0:5], refs[5:10]
    p_all, m_all, v_all, p_block, block, p_rows, m_rows, v_rows, sems, out_sems = refs[-10:]
    core = lax.axis_index("gz_1")
    rows = pl.ds(start, count)

    def copies(p_ref, ref, lanes, slot):
        here = pl.ds(slot * BLOCK, BLOCK)
        return (
            pltpu.make_async_copy(ref.at[:, lanes], block.at[:, here], sems.at[0, slot]),
            pltpu.make_async_copy(p_ref.at[rows, lanes], p_block.at[:, here], sems.at[1, slot]),
        )

    def gather(below_above, received):
        for slot in range(BLOCKS):
            at = jnp.maximum(place[0, slot] - 1, 0)
            part = at // BLOCKS
            lanes = pl.ds(pl.multiple_of((at % BLOCKS) * BLOCK, BLOCK), BLOCK)
            for which, source in enumerate((0, below_above, received)):

                @pl.when(part == which)
                def _(source=source, lanes=lanes, slot=slot):
                    for copy in copies(p_parts[source], parts[source], lanes, slot):
                        copy.start()

    @pl.when(core == 0)
    def _():
        gather(1, 3)

    @pl.when(core == 1)
    def _():
        gather(2, 4)

    factor = clip[0, 0]
    for slot in range(BLOCKS):
        here = pl.ds(slot * BLOCK, BLOCK)
        for copy in copies(p_parts[0], parts[0], pl.ds(0, BLOCK), slot):
            copy.wait()
        second = block[2 * count : 3 * count, here]
        kept = (second > 0.0) & (place[0, slot] > 0)
        clipped = factor * block[0:count, here]
        first = beta_one * block[count : 2 * count, here] + (1.0 - beta_one) * clipped
        second = beta_two * second + (1.0 - beta_two) * clipped * clipped
        updated = p_block[:, here] - learn_rate * (first / correct_one) / (
            jnp.sqrt(second / correct_two) + adam_eps
        )
        p_rows[:, here] = jnp.where(kept, updated, 0.0)
        m_rows[:, here] = jnp.where(kept, first, 0.0)
        v_rows[:, here] = jnp.where(kept, second, 0.0)
    done = [
        pltpu.make_async_copy(rows_ref, whole.at[rows, :], out_sems.at[i])
        for i, (rows_ref, whole) in enumerate(((p_rows, p_all), (m_rows, m_all), (v_rows, v_all)))
    ]
    for copy in done:
        copy.start()
    for copy in done:
        copy.wait()


def update_rows(start, count, place, clip, p_parts, parts, outs, out_type):
    operands = (place, clip, *p_parts, *parts, *outs)
    width = BLOCKS * BLOCK
    return pl.pallas_call(
        lambda *refs: update_kernel(start, count, *refs),
        out_shape=(out_type,) * 3,
        in_specs=[SMEM, SMEM] + [ANY] * (len(operands) - 2),
        out_specs=(ANY,) * 3,
        input_output_aliases={12 + i: i for i in range(len(outs))},
        scratch_shapes=[
            pltpu.VMEM((count, width), jnp.float32),
            pltpu.VMEM((3 * count, width), jnp.float32),
            *[pltpu.VMEM((count, width), jnp.float32)] * 3,
            pltpu.SemaphoreType.DMA((2, BLOCKS)),
            pltpu.SemaphoreType.DMA((3,)),
        ],
        compiler_params=pltpu.CompilerParams(vmem_limit_bytes=8 * 1024 * 1024),
        cost_estimate=pl.CostEstimate(flops=10000000, bytes_accessed=2000000, transcendentals=0),
        name="update",
    )(*operands)


def shards(params, gradients, moment_one, moment_two, keep_mask):
    row_count = params.shape[1]
    f32 = jnp.float32
    small = pltpu.CompilerParams(vmem_limit_bytes=1024 * 1024)

    def moved(name, x):
        def sent(first, stride):
            return lax.ppermute(x, AXES, [(d, d - 2) for d in range(first, DEVICES, stride)])

        if name == LAST:
            even, odd = sent(2, 2), sent(3, 2)
        else:
            even = odd = sent(2, 1)
        below = lax.ppermute(x, "gz_1", [(1, 0)])
        above = lax.ppermute(even, "gz_1", [(0, 1)])
        return x, below, above, even, odd

    pairs, *own = pl.pallas_call(
        pack_kernel,
        out_shape=(
            jax.ShapeDtypeStruct((8, 1, BLOCK), f32),
            *[jax.ShapeDtypeStruct((3 * count, row_count), f32) for _, count in CHUNKS],
        ),
        in_specs=[VMEM] * 4,
        out_specs=(VMEM,) * (1 + len(CHUNKS)),
        name="pack",
    )(gradients, moment_one, moment_two, keep_mask.reshape(BLOCKS, BLOCK))

    near = lax.all_to_all(pairs, NEAR, 0, 0, tiled=True)
    lines = pl.pallas_call(
        line_kernel,
        out_shape=jax.ShapeDtypeStruct((32, 1, BLOCK), f32),
        compiler_params=small,
        name="line",
    )(near)
    far = lax.all_to_all(lines, FAR, 0, 0, tiled=True)
    place, clip, rms = pl.pallas_call(
        table_kernel,
        out_shape=(
            jax.ShapeDtypeStruct((1, BLOCK), jnp.int32),
            jax.ShapeDtypeStruct((1, BLOCK), f32),
            jax.ShapeDtypeStruct((1, 1), f32),
        ),
        compiler_params=small,
        name="table",
    )(near, far)

    out_type = jax.ShapeDtypeStruct(params.shape, f32)
    p_parts = moved("p", params)
    outs = ()
    for i, (start, count) in enumerate(CHUNKS):
        parts = moved(str(i), own[i])
        outs = update_rows(start, count, place, clip, p_parts, parts, outs, out_type)
    return (*outs, rms.reshape(()))


def solution(mesh):
    split = Mesh(mesh.devices.reshape(mesh.shape["gx"], mesh.shape["gy"], 4, 2), AXES)
    spec = P(None, AXES)

    return jax.shard_map(
        shards,
        mesh=split,
        in_specs=(spec, spec, spec, spec, P(AXES)),
        out_specs=(spec, spec, spec, P()),
        check_vma=False,
    )
```

```python
import jax
import jax.numpy as jnp
from jax import lax
from jax.experimental import pallas as pl
from jax.experimental.pallas import tpu as pltpu
from jax.sharding import Mesh
from jax.sharding import PartitionSpec as P


FEATURES = 59
BLOCK = 128
BLOCKS = 16
HALF = 4
STEP = 10
DEVICES = 256
AXES = ("gx", "gy", "gz_0", "gz_1")
NEAR = ("gz_0", "gz_1")
FAR = ("gx", "gy")
CHUNKS = ((32, 27), (0, 32))
LAST = "1"

beta_one = 0.9
beta_two = 0.999
learn_rate = 0.05
adam_eps = 1e-08
clip_rms = 1.0
correct_one = 1.0 - beta_one**STEP
correct_two = 1.0 - beta_two**STEP

ANY = pl.BlockSpec(memory_space=pl.ANY)
SMEM = pl.BlockSpec(memory_space=pltpu.SMEM)
VMEM = pl.BlockSpec(memory_space=pltpu.VMEM)


def pack_kernel(g_ref, m_ref, v_ref, mask_ref, pair_ref, *chunks):
    grads = g_ref[...]
    square = jnp.sum(grads * grads)
    alive = (jnp.max(mask_ref[...], axis=1, keepdims=True) > 0).astype(jnp.float32)
    lane = lax.broadcasted_iota(jnp.int32, (BLOCKS, BLOCK), 1)
    block = lax.broadcasted_iota(jnp.int32, (BLOCKS, BLOCK), 0)
    chosen = (lane == block + 2) | (lane == 1)
    row = jnp.sum(jnp.where(chosen, alive, 0.0), axis=0, keepdims=True)
    first_lane = lax.broadcasted_iota(jnp.int32, (1, BLOCK), 1)
    row = jnp.where(first_lane == 0, square, row)
    pair_ref[...] = jnp.broadcast_to(row[None], pair_ref.shape)
    for (start, count), out in zip(CHUNKS, chunks):
        rows = slice(start, start + count)
        out[0:count, :] = g_ref[rows, :]
        out[count : 2 * count, :] = m_ref[rows, :]
    for b in range(BLOCKS):
        here = slice(b * BLOCK, (b + 1) * BLOCK)
        kept = mask_ref[b : b + 1, :] > 0
        for (start, count), out in zip(CHUNKS, chunks):
            value = v_ref[start : start + count, here]
            out[2 * count : 3 * count, here] = jnp.where(kept, value, 0.0)


def line_kernel(near_ref, far_ref):
    near = near_ref[:, 0, :]
    lane = lax.broadcasted_iota(jnp.int32, (1, BLOCK), 1)
    total = jnp.sum(near, axis=0, keepdims=True)
    second = pltpu.roll(near[1:2], BLOCKS, 1)
    row = jnp.where(lane < 2 + BLOCKS, near[0:1], second)
    row = jnp.where(lane < 2, total, jnp.where(lane < 2 + 2 * BLOCKS, row, 0.0))
    far_ref[...] = jnp.broadcast_to(row[None], far_ref.shape)


def table_kernel(near_ref, far_ref, place_ref, clip_ref, rms_ref):
    y_core = lax.axis_index("gz_0") * 2 + lax.axis_index("gz_1")
    line = lax.axis_index("gx") * 4 + lax.axis_index("gy")
    near = near_ref[:, 0, :]
    far = far_ref[:, 0, :]
    near_row = lax.broadcasted_iota(jnp.int32, near.shape, 0)
    far_row = lax.broadcasted_iota(jnp.int32, far.shape, 0)
    lane = lax.broadcasted_iota(jnp.int32, (1, BLOCK), 1)

    lower = jnp.sum(jnp.where(near_row < y_core, near, 0.0), axis=0, keepdims=True)
    lower += jnp.sum(jnp.where(far_row < line, far, 0.0), axis=0, keepdims=True)
    lower = jnp.sum(jnp.where(lane == 1, lower, 0.0), axis=1, keepdims=True)
    total = jnp.sum(far, axis=0, keepdims=True)
    total = jnp.sum(jnp.where(lane == 0, total, 0.0), axis=1, keepdims=True)
    rms = jnp.sqrt(total / (FEATURES * BLOCKS * BLOCK * DEVICES))
    clip = jnp.minimum(1.0, clip_rms / (rms + 1e-06))
    clip_ref[...] = jnp.broadcast_to(clip, clip_ref.shape)
    rms_ref[...] = rms

    def near_flags(device):
        return jnp.sum(jnp.where(near_row == device, near, 0.0), axis=0, keepdims=True)

    after = jnp.sum(jnp.where(far_row == line + 1, far, 0.0), axis=0, keepdims=True)
    later = pltpu.roll(after, BLOCK - BLOCKS, 1)
    own = near_flags(y_core)
    middle = jnp.where(y_core < 7, near_flags(y_core + 1), after)
    last = jnp.where(y_core < 6, near_flags(y_core + 2), jnp.where(y_core == 6, after, later))
    flags = jnp.where(
        lane < BLOCKS,
        pltpu.roll(own, BLOCK - 2, 1),
        jnp.where(
            lane < 2 * BLOCKS, pltpu.roll(middle, BLOCKS - 2, 1), pltpu.roll(last, 2 * BLOCKS - 2, 1)
        ),
    )
    window = (3 * BLOCKS, BLOCK)
    flags = jnp.broadcast_to(flags, window)
    row = lax.broadcasted_iota(jnp.int32, window, 0)
    column = lax.broadcasted_iota(jnp.int32, window, 1)
    rank = jnp.sum(jnp.where(column < row, flags, 0.0), axis=1, keepdims=True)
    alive = jnp.sum(jnp.where(column == row, flags, 0.0), axis=1, keepdims=True)
    device = line * 8 + y_core
    wanted = (device * BLOCKS).astype(jnp.float32) - lower + column.astype(jnp.float32)
    match = (rank == wanted) & (alive > 0.0)
    place = jnp.sum(jnp.where(match, row + 1, 0), axis=0, keepdims=True)
    place_ref[...] = place


def update_kernel(start, count, place, clip, *refs):
    p_parts, parts = refs[0:5], refs[5:10]
    p_all, m_all, v_all, p_block, block, p_rows, m_rows, v_rows, sems, out_sems = refs[-10:]
    core = lax.axis_index("gz_1")
    rows = pl.ds(start, count)

    def copies(p_ref, ref, lanes, slot):
        here = pl.ds(slot * BLOCK, BLOCK)
        return (
            pltpu.make_async_copy(ref.at[:, lanes], block.at[:, here], sems.at[0, slot]),
            pltpu.make_async_copy(p_ref.at[rows, lanes], p_block.at[:, here], sems.at[1, slot]),
        )

    def gather(below_above, received):
        for slot in range(BLOCKS):
            at = jnp.maximum(place[0, slot] - 1, 0)
            part = at // BLOCKS
            lanes = pl.ds(pl.multiple_of((at % BLOCKS) * BLOCK, BLOCK), BLOCK)
            for which, source in enumerate((0, below_above, received)):

                @pl.when(part == which)
                def _(source=source, lanes=lanes, slot=slot):
                    for copy in copies(p_parts[source], parts[source], lanes, slot):
                        copy.start()

    @pl.when(core == 0)
    def _():
        gather(1, 3)

    @pl.when(core == 1)
    def _():
        gather(2, 4)

    factor = clip[0, 0]
    leaving = []
    for slot in range(BLOCKS):
        here = pl.ds(slot * BLOCK, BLOCK)
        if slot % HALF == 0:
            for ready in range(slot, slot + HALF):
                for copy in copies(p_parts[0], parts[0], pl.ds(0, BLOCK), ready):
                    copy.wait()
        second = block[2 * count : 3 * count, here]
        kept = (second > 0.0) & (place[0, slot] > 0)
        clipped = factor * block[0:count, here]
        first = beta_one * block[count : 2 * count, here] + (1.0 - beta_one) * clipped
        second = beta_two * second + (1.0 - beta_two) * clipped * clipped
        updated = p_block[:, here] - learn_rate * (first / correct_one) / (
            jnp.sqrt(second / correct_two) + adam_eps
        )
        p_rows[:, here] = jnp.where(kept, updated, 0.0)
        m_rows[:, here] = jnp.where(kept, first, 0.0)
        v_rows[:, here] = jnp.where(kept, second, 0.0)
        if slot % HALF == HALF - 1:
            columns = pl.ds((slot // HALF) * HALF * BLOCK, HALF * BLOCK)
            for i, (mine, whole) in enumerate(((p_rows, p_all), (m_rows, m_all), (v_rows, v_all))):
                copy = pltpu.make_async_copy(
                    mine.at[:, columns], whole.at[rows, columns], out_sems.at[slot // HALF, i]
                )
                copy.start()
                leaving.append(copy)
    for copy in leaving:
        copy.wait()


def update_rows(start, count, place, clip, p_parts, parts, outs, out_type):
    operands = (place, clip, *p_parts, *parts, *outs)
    width = BLOCKS * BLOCK
    return pl.pallas_call(
        lambda *refs: update_kernel(start, count, *refs),
        out_shape=(out_type,) * 3,
        in_specs=[SMEM, SMEM] + [ANY] * (len(operands) - 2),
        out_specs=(ANY,) * 3,
        input_output_aliases={12 + i: i for i in range(len(outs))},
        scratch_shapes=[
            pltpu.VMEM((count, width), jnp.float32),
            pltpu.VMEM((3 * count, width), jnp.float32),
            *[pltpu.VMEM((count, width), jnp.float32)] * 3,
            pltpu.SemaphoreType.DMA((2, BLOCKS)),
            pltpu.SemaphoreType.DMA((BLOCKS // HALF, 3)),
        ],
        compiler_params=pltpu.CompilerParams(vmem_limit_bytes=8 * 1024 * 1024),
        cost_estimate=pl.CostEstimate(flops=10000000, bytes_accessed=2000000, transcendentals=0),
        name="update",
    )(*operands)


def shards(params, gradients, moment_one, moment_two, keep_mask):
    row_count = params.shape[1]
    f32 = jnp.float32
    small = pltpu.CompilerParams(vmem_limit_bytes=1024 * 1024)

    def moved(name, x):
        def sent(first, stride):
            return lax.ppermute(x, AXES, [(d, d - 2) for d in range(first, DEVICES, stride)])

        if name == LAST:
            even, odd = sent(2, 2), sent(3, 2)
        else:
            even = odd = sent(2, 1)
        below = lax.ppermute(x, "gz_1", [(1, 0)])
        above = lax.ppermute(even, "gz_1", [(0, 1)])
        return x, below, above, even, odd

    pairs, *own = pl.pallas_call(
        pack_kernel,
        out_shape=(
            jax.ShapeDtypeStruct((8, 1, BLOCK), f32),
            *[jax.ShapeDtypeStruct((3 * count, row_count), f32) for _, count in CHUNKS],
        ),
        in_specs=[VMEM] * 4,
        out_specs=(VMEM,) * (1 + len(CHUNKS)),
        name="pack",
    )(gradients, moment_one, moment_two, keep_mask.reshape(BLOCKS, BLOCK))

    near = lax.all_to_all(pairs, NEAR, 0, 0, tiled=True)
    lines = pl.pallas_call(
        line_kernel,
        out_shape=jax.ShapeDtypeStruct((32, 1, BLOCK), f32),
        compiler_params=small,
        name="line",
    )(near)
    far = lax.all_to_all(lines, FAR, 0, 0, tiled=True)
    place, clip, rms = pl.pallas_call(
        table_kernel,
        out_shape=(
            jax.ShapeDtypeStruct((1, BLOCK), jnp.int32),
            jax.ShapeDtypeStruct((1, BLOCK), f32),
            jax.ShapeDtypeStruct((1, 1), f32),
        ),
        compiler_params=small,
        name="table",
    )(near, far)

    out_type = jax.ShapeDtypeStruct(params.shape, f32)
    p_parts = moved("p", params)
    outs = ()
    for i, (start, count) in enumerate(CHUNKS):
        parts = moved(str(i), own[i])
        outs = update_rows(start, count, place, clip, p_parts, parts, outs, out_type)
    return (*outs, rms.reshape(()))


def solution(mesh):
    split = Mesh(mesh.devices.reshape(mesh.shape["gx"], mesh.shape["gy"], 4, 2), AXES)
    spec = P(None, AXES)

    return jax.shard_map(
        shards,
        mesh=split,
        in_specs=(spec, spec, spec, spec, P(AXES)),
        out_specs=(spec, spec, spec, P()),
        check_vma=False,
    )
```

```python
import jax
import jax.numpy as jnp
from jax import lax
from jax.experimental import pallas as pl
from jax.experimental.pallas import tpu as pltpu
from jax.sharding import Mesh
from jax.sharding import PartitionSpec as P


FEATURES = 59
BLOCK = 128
BLOCKS = 16
HALF = 4
STEP = 10
DEVICES = 256
AXES = ("gx", "gy", "gz_0", "gz_1")
NEAR = ("gz_0", "gz_1")
FAR = ("gx", "gy")
CHUNKS = ((32, 27), (0, 32))
LAST = "1"

beta_one = 0.9
beta_two = 0.999
learn_rate = 0.05
adam_eps = 1e-08
clip_rms = 1.0
correct_one = 1.0 - beta_one**STEP
correct_two = 1.0 - beta_two**STEP

ANY = pl.BlockSpec(memory_space=pl.ANY)
SMEM = pl.BlockSpec(memory_space=pltpu.SMEM)
VMEM = pl.BlockSpec(memory_space=pltpu.VMEM)


def pack_kernel(g_ref, m_ref, v_ref, mask_ref, pair_ref, *chunks):
    grads = g_ref[...]
    square = jnp.sum(grads * grads)
    alive = (jnp.max(mask_ref[...], axis=1, keepdims=True) > 0).astype(jnp.float32)
    lane = lax.broadcasted_iota(jnp.int32, (BLOCKS, BLOCK), 1)
    block = lax.broadcasted_iota(jnp.int32, (BLOCKS, BLOCK), 0)
    chosen = (lane == block + 2) | (lane == 1)
    row = jnp.sum(jnp.where(chosen, alive, 0.0), axis=0, keepdims=True)
    first_lane = lax.broadcasted_iota(jnp.int32, (1, BLOCK), 1)
    row = jnp.where(first_lane == 0, square, row)
    pair_ref[...] = jnp.broadcast_to(row[None], pair_ref.shape)
    for (start, count), out in zip(CHUNKS, chunks):
        rows = slice(start, start + count)
        out[0:count, :] = g_ref[rows, :]
        out[count : 2 * count, :] = m_ref[rows, :]
    for b in range(BLOCKS):
        here = slice(b * BLOCK, (b + 1) * BLOCK)
        kept = mask_ref[b : b + 1, :] > 0
        for (start, count), out in zip(CHUNKS, chunks):
            value = v_ref[start : start + count, here]
            out[2 * count : 3 * count, here] = jnp.where(kept, value, 0.0)


def line_kernel(near_ref, far_ref):
    near = near_ref[:, 0, :]
    lane = lax.broadcasted_iota(jnp.int32, (1, BLOCK), 1)
    total = jnp.sum(near, axis=0, keepdims=True)
    second = pltpu.roll(near[1:2], BLOCKS, 1)
    row = jnp.where(lane < 2 + BLOCKS, near[0:1], second)
    row = jnp.where(lane < 2, total, jnp.where(lane < 2 + 2 * BLOCKS, row, 0.0))
    far_ref[...] = jnp.broadcast_to(row[None], far_ref.shape)


def table_kernel(near_ref, far_ref, place_ref, clip_ref, rms_ref):
    y_core = lax.axis_index("gz_0") * 2 + lax.axis_index("gz_1")
    line = lax.axis_index("gx") * 4 + lax.axis_index("gy")
    near = near_ref[:, 0, :]
    far = far_ref[:, 0, :]
    near_row = lax.broadcasted_iota(jnp.int32, near.shape, 0)
    far_row = lax.broadcasted_iota(jnp.int32, far.shape, 0)
    lane = lax.broadcasted_iota(jnp.int32, (1, BLOCK), 1)

    lower = jnp.sum(jnp.where(near_row < y_core, near, 0.0), axis=0, keepdims=True)
    lower += jnp.sum(jnp.where(far_row < line, far, 0.0), axis=0, keepdims=True)
    lower = jnp.sum(jnp.where(lane == 1, lower, 0.0), axis=1, keepdims=True)
    total = jnp.sum(far, axis=0, keepdims=True)
    total = jnp.sum(jnp.where(lane == 0, total, 0.0), axis=1, keepdims=True)
    rms = jnp.sqrt(total / (FEATURES * BLOCKS * BLOCK * DEVICES))
    clip = jnp.minimum(1.0, clip_rms / (rms + 1e-06))
    clip_ref[...] = jnp.broadcast_to(clip, clip_ref.shape)
    rms_ref[...] = rms

    def near_flags(device):
        return jnp.sum(jnp.where(near_row == device, near, 0.0), axis=0, keepdims=True)

    after = jnp.sum(jnp.where(far_row == line + 1, far, 0.0), axis=0, keepdims=True)
    later = pltpu.roll(after, BLOCK - BLOCKS, 1)
    own = near_flags(y_core)
    middle = jnp.where(y_core < 7, near_flags(y_core + 1), after)
    last = jnp.where(y_core < 6, near_flags(y_core + 2), jnp.where(y_core == 6, after, later))
    flags = jnp.where(
        lane < BLOCKS,
        pltpu.roll(own, BLOCK - 2, 1),
        jnp.where(
            lane < 2 * BLOCKS, pltpu.roll(middle, BLOCKS - 2, 1), pltpu.roll(last, 2 * BLOCKS - 2, 1)
        ),
    )
    window = (3 * BLOCKS, BLOCK)
    flags = jnp.broadcast_to(flags, window)
    row = lax.broadcasted_iota(jnp.int32, window, 0)
    column = lax.broadcasted_iota(jnp.int32, window, 1)
    rank = jnp.sum(jnp.where(column < row, flags, 0.0), axis=1, keepdims=True)
    alive = jnp.sum(jnp.where(column == row, flags, 0.0), axis=1, keepdims=True)
    device = line * 8 + y_core
    wanted = (device * BLOCKS).astype(jnp.float32) - lower + column.astype(jnp.float32)
    match = (rank == wanted) & (alive > 0.0)
    place = jnp.sum(jnp.where(match, row + 1, 0), axis=0, keepdims=True)
    place_ref[...] = place


def update_kernel(start, count, place, clip, *refs):
    p_parts, parts = refs[0:5], refs[5:10]
    p_all, m_all, v_all, p_block, block, p_rows, m_rows, v_rows, sems, out_sems = refs[-10:]
    core = lax.axis_index("gz_1")
    rows = pl.ds(start, count)

    def copies(p_ref, ref, lanes, slot):
        here = pl.ds(slot * BLOCK, BLOCK)
        return (
            pltpu.make_async_copy(ref.at[:, lanes], block.at[:, here], sems.at[0, slot]),
            pltpu.make_async_copy(p_ref.at[rows, lanes], p_block.at[:, here], sems.at[1, slot]),
        )

    def gather(first, below_above, received):
        for slot in range(first, first + HALF):
            at = jnp.maximum(place[0, slot] - 1, 0)
            lanes = pl.ds(pl.multiple_of((at % BLOCKS) * BLOCK, BLOCK), BLOCK)

            def start(source, lanes=lanes, slot=slot):
                for copy in copies(p_parts[source], parts[source], lanes, slot):
                    copy.start()

            @pl.when(at < BLOCKS)
            def _(start=start):
                start(0)

            @pl.when(at >= BLOCKS)
            def _(start=start, at=at):
                @pl.when(at < 2 * BLOCKS)
                def _():
                    start(below_above)

                @pl.when(at >= 2 * BLOCKS)
                def _():
                    start(received)

    def gather_here(first):
        @pl.when(core == 0)
        def _():
            gather(first, 1, 3)

        @pl.when(core == 1)
        def _():
            gather(first, 2, 4)

    gather_here(0)
    gather_here(HALF)
    factor = clip[0, 0]
    leaving = []
    for slot in range(BLOCKS):
        here = pl.ds(slot * BLOCK, BLOCK)
        if slot % HALF == 0:
            if 0 < slot < BLOCKS - HALF:
                gather_here(slot + HALF)
            for ready in range(slot, slot + HALF):
                for copy in copies(p_parts[0], parts[0], pl.ds(0, BLOCK), ready):
                    copy.wait()
        second = block[2 * count : 3 * count, here]
        kept = (second > 0.0) & (place[0, slot] > 0)
        clipped = factor * block[0:count, here]
        first = beta_one * block[count : 2 * count, here] + (1.0 - beta_one) * clipped
        second = beta_two * second + (1.0 - beta_two) * clipped * clipped
        updated = p_block[:, here] - learn_rate * (first / correct_one) / (
            jnp.sqrt(second / correct_two) + adam_eps
        )
        p_rows[:, here] = jnp.where(kept, updated, 0.0)
        m_rows[:, here] = jnp.where(kept, first, 0.0)
        v_rows[:, here] = jnp.where(kept, second, 0.0)
        if slot % HALF == HALF - 1:
            columns = pl.ds((slot // HALF) * HALF * BLOCK, HALF * BLOCK)
            for i, (mine, whole) in enumerate(((p_rows, p_all), (m_rows, m_all), (v_rows, v_all))):
                copy = pltpu.make_async_copy(
                    mine.at[:, columns], whole.at[rows, columns], out_sems.at[slot // HALF, i]
                )
                copy.start()
                leaving.append(copy)
    for copy in leaving:
        copy.wait()


def update_rows(start, count, place, clip, p_parts, parts, outs, out_type):
    operands = (place, clip, *p_parts, *parts, *outs)
    width = BLOCKS * BLOCK
    return pl.pallas_call(
        lambda *refs: update_kernel(start, count, *refs),
        out_shape=(out_type,) * 3,
        in_specs=[SMEM, SMEM] + [ANY] * (len(operands) - 2),
        out_specs=(ANY,) * 3,
        input_output_aliases={12 + i: i for i in range(len(outs))},
        scratch_shapes=[
            pltpu.VMEM((count, width), jnp.float32),
            pltpu.VMEM((3 * count, width), jnp.float32),
            *[pltpu.VMEM((count, width), jnp.float32)] * 3,
            pltpu.SemaphoreType.DMA((2, BLOCKS)),
            pltpu.SemaphoreType.DMA((BLOCKS // HALF, 3)),
        ],
        compiler_params=pltpu.CompilerParams(vmem_limit_bytes=8 * 1024 * 1024),
        cost_estimate=pl.CostEstimate(flops=10000000, bytes_accessed=2000000, transcendentals=0),
        name="update",
    )(*operands)


def shards(params, gradients, moment_one, moment_two, keep_mask):
    row_count = params.shape[1]
    f32 = jnp.float32
    small = pltpu.CompilerParams(vmem_limit_bytes=1024 * 1024)

    def moved(name, x):
        def sent(first, stride):
            return lax.ppermute(x, AXES, [(d, d - 2) for d in range(first, DEVICES, stride)])

        if name == LAST:
            even, odd = sent(2, 2), sent(3, 2)
        else:
            even = odd = sent(2, 1)
        below = lax.ppermute(x, "gz_1", [(1, 0)])
        above = lax.ppermute(even, "gz_1", [(0, 1)])
        return x, below, above, even, odd

    pairs, *own = pl.pallas_call(
        pack_kernel,
        out_shape=(
            jax.ShapeDtypeStruct((8, 1, BLOCK), f32),
            *[jax.ShapeDtypeStruct((3 * count, row_count), f32) for _, count in CHUNKS],
        ),
        in_specs=[VMEM] * 4,
        out_specs=(VMEM,) * (1 + len(CHUNKS)),
        name="pack",
    )(gradients, moment_one, moment_two, keep_mask.reshape(BLOCKS, BLOCK))

    near = lax.all_to_all(pairs, NEAR, 0, 0, tiled=True)
    lines = pl.pallas_call(
        line_kernel,
        out_shape=jax.ShapeDtypeStruct((32, 1, BLOCK), f32),
        compiler_params=small,
        name="line",
    )(near)
    far = lax.all_to_all(lines, FAR, 0, 0, tiled=True)
    place, clip, rms = pl.pallas_call(
        table_kernel,
        out_shape=(
            jax.ShapeDtypeStruct((1, BLOCK), jnp.int32),
            jax.ShapeDtypeStruct((1, BLOCK), f32),
            jax.ShapeDtypeStruct((1, 1), f32),
        ),
        compiler_params=small,
        name="table",
    )(near, far)

    out_type = jax.ShapeDtypeStruct(params.shape, f32)
    p_parts = moved("p", params)
    outs = ()
    for i, (start, count) in enumerate(CHUNKS):
        parts = moved(str(i), own[i])
        outs = update_rows(start, count, place, clip, p_parts, parts, outs, out_type)
    return (*outs, rms.reshape(()))


def solution(mesh):
    split = Mesh(mesh.devices.reshape(mesh.shape["gx"], mesh.shape["gy"], 4, 2), AXES)
    spec = P(None, AXES)

    return jax.shard_map(
        shards,
        mesh=split,
        in_specs=(spec, spec, spec, spec, P(AXES)),
        out_specs=(spec, spec, spec, P()),
        check_vma=False,
    )
```
